32 devices in a mesh: member: 2 (over y), lat: 16 (over z, x, core).
Axes of the slice: x: 2, y: 2, z: 4, core: 2. Of those that a mesh axis runs over, the one named last changes fastest.
Arguments:
- tracers: float32 [60, 4, 64, 1440], P('member', None, 'lat'), parts along dimension 0, may hold values from -6 to 6
- currents: float32 [4, 4, 64, 1440], P('member', None, 'lat'), parts along dimension 0, may hold values from -0.4 to 0.4
- column_levels: int32 [128, 1440], P(('member', 'lat')), parts along dimension 0, may hold values from 0 to 4
Outputs:
- advected: float32 [60, 4, 64, 1440], P('member', None, 'lat'), parts along dimension 0
The draws below stay inside these ranges and needn't reach their ends.
There are 2 independent parts, one for each index of `member`. The reference program is written for one: setup_inputs(seed, part) draws one part's arguments, and reference() takes and returns one part's arrays. A program takes and returns all parts, laid end to end along the dimension named above; each array names one. Nothing has to cross between parts.
All inputs are finite; a program needn't handle non-finite values.
Results may differ from the reference program's by a relative error of at most 0.00002.
Values sent between devices are 32-bit elements; how exact they have to be, the bound alone decides.
A program may use at most 64 MiB of HBM per device.

```python
import jax
import jax.numpy as jnp

TRACERS = 30
LEVELS = 4
NLON = 1440
NLAT = 64


def place_ends(values, own_key, least, top_value):
    longest = values.shape.index(max(values.shape))
    spots = []
    for shift in (0, 1):
        where = [jax.random.randint(jax.random.fold_in(own_key, axis), (), 0, length) for axis, length in enumerate(values.shape)]
        where[longest] = (where[longest] + shift) % values.shape[longest]
        spots.append(tuple(where))
    return values.at[spots[0]].set(least).at[spots[1]].set(top_value)


def shard_levels(rng, shape, shards, least, high):
    level, own = 1.0, jax.random.fold_in(rng, 6)
    for position, parts in shards:
        steps = jnp.exp(jax.random.uniform(jax.random.fold_in(own, position), (parts,), jnp.float32, least / len(shards), high / len(shards)))
        level = level * jnp.repeat(steps, shape[position] // parts).reshape([-1 if axis == position else 1 for axis in range(len(shape))])
    return level


def scatter_about(rng, dims, spread, limit, pieces=(), kind=jnp.bfloat16):
    gain = shard_levels(rng, dims, pieces, -0.22, 0.18) if pieces else 1.0
    result = jax.random.normal(rng, dims, jnp.float32) * spread * gain
    return jnp.minimum(jnp.maximum(result, -limit), limit).astype(kind)


def setup_inputs(seed: int = 0, part: int = 0) -> dict:
    splits = jax.random.split(jax.random.key(seed), 4)
    part_splits = jax.random.split(jax.random.fold_in(splits[3], part), 4)
    tracers = scatter_about(part_splits[0], (TRACERS, LEVELS, NLAT, NLON), 1.0, 6.0, ((2, 16),), jnp.float32)
    currents = jnp.clip(jax.random.uniform(part_splits[1], (2, LEVELS, NLAT, NLON), jnp.float32, -0.4, 0.4) * shard_levels(part_splits[1], (2, LEVELS, NLAT, NLON), ((2, 16),), -0.4, 0.0), -0.4, 0.4)
    column_levels = place_ends(jax.random.randint(part_splits[2], (NLAT, NLON), 0, LEVELS + 1), jax.random.fold_in(part_splits[2], 1), 0, LEVELS).astype(jnp.int32)
    return {"tracers": tracers, "currents": currents, "column_levels": column_levels}


def face_flux(courant, before, left, right, after):
    central = courant * (7.0 * (left + right) - (before + after)) / 12.0
    upwind = jnp.abs(courant) * (3.0 * (right - left) - (after - before)) / 12.0
    return central - upwind


def advect_section(padded, east_pad, north_pad, wet_pad):
    rows = padded.shape[-2] - 4
    field = padded[..., 2:-2, :]
    east = east_pad[:, 1:-1]
    wet_rows = wet_pad[:, 1:-1]
    east_face = 0.5 * (east + jnp.roll(east, -1, -1))
    east_open = wet_rows * jnp.roll(wet_rows, -1, -1)
    east_flux = east_open * face_flux(east_face, jnp.roll(field, 1, -1), field, jnp.roll(field, -1, -1), jnp.roll(field, -2, -1))
    east_div = east_flux - jnp.roll(east_flux, 1, -1)
    north_face = 0.5 * (north_pad[:, :-1] + north_pad[:, 1:])
    north_open = wet_pad[:, :-1] * wet_pad[:, 1:]
    north_flux = north_open * face_flux(north_face, padded[..., 0:rows + 1, :], padded[..., 1:rows + 2, :], padded[..., 2:rows + 3, :], padded[..., 3:rows + 4, :])
    north_div = north_flux[..., 1:, :] - north_flux[..., :-1, :]
    return field - east_div - north_div


def extend(field, width, factor):
    south = jnp.zeros(field.shape[:-2] + (width, field.shape[-1]), jnp.float32)
    north = factor * jnp.flip(field[..., field.shape[-2] - width:, :], axis=(-2, -1))
    return jnp.concatenate([south, field, north], axis=-2)


def reference(tracers, currents, column_levels):
    levels = jnp.arange(tracers.shape[1], dtype=jnp.int32)
    wet = (levels[:, None, None] < column_levels[None]).astype(jnp.float32)
    east_pad = extend(currents[0], 1, -1.0)
    north_pad = extend(currents[1], 1, -1.0)
    wet_pad = extend(wet, 1, 1.0)
    start = tracers * wet
    first = advect_section(extend(start, 2, 1.0), east_pad, north_pad, wet_pad) * wet
    second = advect_section(extend(first, 2, 1.0), east_pad, north_pad, wet_pad)
    return 0.5 * (start + second) * wet
```

```python
import functools

import jax
import jax.numpy as jnp
from jax import lax
from jax.experimental import pallas as pl
from jax.experimental.pallas import tpu as pltpu
from jax.sharding import PartitionSpec as P

LANES = 128
WRAP = 4
MESH = pl.DeviceIdType.MESH


def wrapped(x, width):
    n = x.shape[-1]
    gap = jnp.zeros(x.shape[:-1] + (width - n - 2 * WRAP,), x.dtype)
    return jnp.concatenate([x, x[..., :WRAP], gap, x[..., n - WRAP :]], axis=-1)


def face_terms(c, opened):
    c = c * opened * (1.0 / 12.0)
    m = jnp.abs(c)
    return -c - m, 7.0 * c + 3.0 * m, 7.0 * c - 3.0 * m, m - c


def mirrored(tiles, nlon):
    count = len(tiles)
    rest = nlon % LANES
    row = lax.broadcasted_iota(jnp.int32, (LANES, LANES), 0)
    col = lax.broadcasted_iota(jnp.int32, (LANES, LANES), 1)
    near = jnp.where((row + col == rest - 1), 1.0, 0.0).astype(jnp.float32)
    far = jnp.where((row + col == LANES + rest - 1), 1.0, 0.0).astype(jnp.float32)
    dot = functools.partial(
        jnp.dot, precision=lax.Precision.HIGHEST, preferred_element_type=jnp.float32
    )
    return [
        dot(tiles[(count - 1 - q) % count], near) + dot(tiles[(count - 2 - q) % count], far)
        for q in range(count)
    ]


def kernel(
    nlon, levels, start_ref, flow_ref, lev_ref, out_ref,
    lo, hi, flow_lo, flow_hi, lev_lo, lev_hi, coef, wets, first,
    send_up, recv_up, send_dn, recv_dn, fsend, frecv,
):
    lat = lax.axis_size("lat")
    me = lax.axis_index("lat")
    width = start_ref.shape[-1]
    rows = start_ref.shape[0]
    chunks = start_ref.shape[1] // 8
    has_lo = me > 0
    has_hi = me < lat - 1

    barrier = pltpu.get_barrier_semaphore()

    @pl.when(has_lo)
    def _():
        pl.semaphore_signal(barrier, inc=1, device_id={"lat": me - 1}, device_id_type=MESH)

    @pl.when(has_hi)
    def _():
        pl.semaphore_signal(barrier, inc=1, device_id={"lat": me + 1}, device_id_type=MESH)

    @pl.when(has_lo & has_hi)
    def _():
        pl.semaphore_wait(barrier, 2)

    @pl.when(jnp.logical_not(has_lo & has_hi))
    def _():
        pl.semaphore_wait(barrier, 1)

    def remote(src, dst, s, r, target):
        return pltpu.make_async_remote_copy(
            src_ref=src, dst_ref=dst, send_sem=s, recv_sem=r,
            device_id={"lat": target}, device_id_type=MESH,
        )

    def flows(up):
        far = me + 1 if up else me - 1
        base = 0 if up else 3
        n = rows - 1
        part = pl.ds(1, n) if up else pl.ds(0, n)
        dst_f, dst_l = (flow_lo, lev_lo) if up else (flow_hi, lev_hi)
        two = pl.ds(rows - 2, 2) if up else pl.ds(0, 2)
        return [
            remote(lev_ref.at[part], dst_l.at[part], fsend.at[base], frecv.at[base], far),
            remote(flow_ref.at[1, part], dst_f.at[1, part], fsend.at[base + 1], frecv.at[base + 1], far),
            remote(flow_ref.at[0, two], dst_f.at[0, two], fsend.at[base + 2], frecv.at[base + 2], far),
        ]

    def chunk(up, g):
        part = pl.ds(pl.multiple_of(g * 8, 8), 8)
        if up:
            return remote(start_ref.at[:, part], lo.at[:, part], send_up.at[g], recv_up.at[g], me + 1)
        return remote(start_ref.at[:, part], hi.at[:, part], send_dn.at[g], recv_dn.at[g], me - 1)

    @pl.when(has_hi)
    def _():
        for c in flows(True):
            c.start()

    @pl.when(has_lo)
    def _():
        for c in flows(False):
            c.start()

    def begin(g, carry):
        @pl.when(has_hi)
        def _():
            chunk(True, g).start()

        @pl.when(has_lo)
        def _():
            chunk(False, g).start()

        return carry

    lax.fori_loop(0, chunks, begin, 0)

    @pl.when(jnp.logical_not(has_lo))
    def _():
        flow_lo[...] = jnp.zeros_like(flow_lo)
        lev_lo[...] = jnp.zeros_like(lev_lo)
        lo[...] = jnp.zeros_like(lo)

    def tiles_of(x):
        return [x[:, q * LANES : (q + 1) * LANES] for q in range(width // LANES)]

    @pl.when(jnp.logical_not(has_hi))
    def _():
        for k in range(rows):
            src = rows - 1 - k
            piece = jnp.concatenate([flow_ref[0, src], flow_ref[1, src]], axis=0)
            for q, t in enumerate(mirrored(tiles_of(piece), nlon)):
                lane = pl.ds(q * LANES, LANES)
                flow_hi[0, k, :, lane] = -t[:levels]
                flow_hi[1, k, :, lane] = -t[levels:]
            lev = jnp.broadcast_to(lev_ref[src], (8, width))
            for q, t in enumerate(mirrored(tiles_of(lev), nlon)):
                lev_hi[k, :, pl.ds(q * LANES, LANES)] = t[:1]

        def fold(g, carry):
            part = pl.ds(pl.multiple_of(g * 8, 8), 8)
            x = jnp.concatenate([start_ref[rows - 1 - k, part, :] for k in range(rows)], axis=0)
            for q, t in enumerate(mirrored(tiles_of(x), nlon)):
                for k in range(rows):
                    hi[k, part, pl.ds(q * LANES, LANES)] = t[8 * k : 8 * k + 8]
            return carry

        lax.fori_loop(0, chunks, fold, 0)

    @pl.when(has_lo)
    def _():
        for c in flows(True):
            c.wait_recv()

    @pl.when(has_hi)
    def _():
        for c in flows(False):
            c.wait_recv()

    def pick(low, own, high, j):
        if j < 0:
            return low, j + rows
        if j < rows:
            return own, j
        return high, j - rows

    def shift(x, by):
        return pltpu.roll(x, (-by) % width, 1)

    ranks = lax.rem(lax.broadcasted_iota(jnp.int32, (8, width), 0), levels).astype(jnp.float32)

    def wet_row(j):
        ref, k = pick(lev_lo, lev_ref, lev_hi, j)
        return jnp.where(ranks < jnp.broadcast_to(ref[k], (8, width)), 1.0, 0.0)

    def flow_row(which, j):
        ref, k = pick(flow_lo, flow_ref, flow_hi, j)
        return jnp.concatenate([ref[which, k]] * (8 // levels), axis=0)

    def north_face(j):
        return face_terms(
            0.5 * (flow_row(1, j) + flow_row(1, j + 1)), wet_row(j) * wet_row(j + 1)
        )

    below = north_face(-3)
    for k in range(rows + 4):
        j = k - 2
        wet = wet_row(j)
        u = flow_row(0, j)
        ea, eb, ed, ee = face_terms(0.5 * (u + shift(u, 1)), wet * shift(wet, 1))
        above = north_face(j)
        coef[k, 0] = shift(ea, -1)
        coef[k, 1] = shift(eb, -1) - ea
        coef[k, 2] = shift(ee, -1) - ed
        coef[k, 3] = -ee
        coef[k, 4] = below[0]
        coef[k, 5] = below[1] - above[0]
        coef[k, 6] = below[3] - above[2]
        coef[k, 7] = -above[3]
        coef[k, 8] = 1.0 - eb + shift(ed, -1) - above[1] + below[2]
        wets[k] = wet
        below = above

    def section(get, k):
        f = get(0)
        total = coef[k, 8] * f
        total += coef[k, 0] * shift(f, -2)
        total += coef[k, 1] * shift(f, -1)
        total += coef[k, 2] * shift(f, 1)
        total += coef[k, 3] * shift(f, 2)
        total += coef[k, 4] * get(-2)
        total += coef[k, 5] * get(-1)
        total += coef[k, 6] * get(1)
        total += coef[k, 7] * get(2)
        return total

    def step(g, carry):
        @pl.when(has_lo)
        def _():
            chunk(True, g).wait_recv()

        @pl.when(has_hi)
        def _():
            chunk(False, g).wait_recv()

        part = pl.ds(pl.multiple_of(g * 8, 8), 8)

        def start_row(j):
            ref, k = pick(lo, start_ref, hi, j)
            return ref[k, part, :]

        for k in range(rows + 4):
            first[k] = section(lambda d: start_row(k - 2 + d), k) * wets[k]
        for j in range(rows):
            second = section(lambda d: first[j + 2 + d], j + 2)
            value = 0.5 * (start_ref[j, part, :] + second) * wets[j + 2]
            out_ref[j, part, :] = value[:, :nlon]
        return carry

    lax.fori_loop(0, chunks, step, 0)

    @pl.when(has_hi)
    def _():
        for c in flows(True):
            c.wait_send()

    @pl.when(has_lo)
    def _():
        for c in flows(False):
            c.wait_send()

    def finish(g, carry):
        @pl.when(has_hi)
        def _():
            chunk(True, g).wait_send()

        @pl.when(has_lo)
        def _():
            chunk(False, g).wait_send()

        return carry

    lax.fori_loop(0, chunks, finish, 0)


def shards(tracers, currents, column_levels):
    count, levels, rows, nlon = tracers.shape
    width = -(-(nlon + 2 * WRAP) // LANES) * LANES
    ranks = jnp.arange(levels, dtype=jnp.int32)
    wet = (ranks[:, None, None] < column_levels[None]).astype(jnp.float32)
    start = jnp.transpose(tracers * wet, (2, 0, 1, 3)).reshape(rows, count * levels, nlon)
    start = wrapped(start, width)
    flow = wrapped(jnp.transpose(currents, (0, 2, 1, 3)), width)
    lev = wrapped(column_levels.astype(jnp.float32), width)[:, None, :]
    chunks = count * levels // 8
    vmem = pl.BlockSpec(memory_space=pltpu.VMEM)
    dma = pltpu.SemaphoreType.DMA
    out = pl.pallas_call(
        functools.partial(kernel, nlon, levels),
        out_shape=jax.ShapeDtypeStruct((rows, count * levels, nlon), jnp.float32),
        in_specs=[vmem] * 3,
        out_specs=vmem,
        scratch_shapes=[
            pltpu.VMEM(start.shape, jnp.float32),
            pltpu.VMEM(start.shape, jnp.float32),
            pltpu.VMEM(flow.shape, jnp.float32),
            pltpu.VMEM(flow.shape, jnp.float32),
            pltpu.VMEM(lev.shape, jnp.float32),
            pltpu.VMEM(lev.shape, jnp.float32),
            pltpu.VMEM((rows + 4, 9, 8, width), jnp.float32),
            pltpu.VMEM((rows + 4, 8, width), jnp.float32),
            pltpu.VMEM((rows + 4, 8, width), jnp.float32),
            dma((chunks,)), dma((chunks,)), dma((chunks,)), dma((chunks,)),
            dma((6,)), dma((6,)),
        ],
        compiler_params=pltpu.CompilerParams(
            collective_id=0, has_side_effects=True, vmem_limit_bytes=60000 * 1024
        ),
    )(start, flow, lev)
    return jnp.transpose(out.reshape(rows, count, levels, nlon), (1, 2, 0, 3))


def solution(mesh):
    in_specs = (
        P("member", None, "lat", None),
        P("member", None, "lat", None),
        P(("member", "lat"), None),
    )
    out_specs = P("member", None, "lat", None)
    return jax.shard_map(shards, mesh=mesh, in_specs=in_specs, out_specs=out_specs, check_vma=False)
```

```python
import functools

import jax
import jax.numpy as jnp
from jax import lax
from jax.experimental import pallas as pl
from jax.experimental.pallas import tpu as pltpu
from jax.sharding import PartitionSpec as P

LANES = 128
WRAP = 4
MESH = pl.DeviceIdType.MESH


def wrapped(x, nlon):
    rest = nlon % LANES
    whole = nlon - rest
    tail = jnp.concatenate([x[:, whole:], x[:, : LANES - rest]], axis=1)
    lane = lax.broadcasted_iota(jnp.int32, tail.shape, 1)
    tail = jnp.where(lane >= LANES - WRAP, pltpu.roll(tail, LANES - rest, 1), tail)
    return jnp.concatenate([x[:, :whole], tail], axis=1)


def face_terms(c, opened):
    c = c * opened * (1.0 / 12.0)
    m = jnp.abs(c)
    return -c - m, 7.0 * c + 3.0 * m, 7.0 * c - 3.0 * m, m - c


def mirrored(tiles, nlon):
    count = len(tiles)
    rest = nlon % LANES
    row = lax.broadcasted_iota(jnp.int32, (LANES, LANES), 0)
    col = lax.broadcasted_iota(jnp.int32, (LANES, LANES), 1)
    near = jnp.where((row + col == rest - 1), 1.0, 0.0).astype(jnp.float32)
    far = jnp.where((row + col == LANES + rest - 1), 1.0, 0.0).astype(jnp.float32)
    dot = functools.partial(
        jnp.dot, precision=lax.Precision.HIGHEST, preferred_element_type=jnp.float32
    )
    return [
        dot(tiles[(count - 1 - q) % count], near) + dot(tiles[(count - 2 - q) % count], far)
        for q in range(count)
    ]


def kernel(
    nlon, levels, start_ref, flow_ref, lev_ref, out_ref,
    lo, hi, flow_lo, flow_hi, lev_lo, lev_hi, coef, wets, field, first,
    send_up, recv_up, send_dn, recv_dn, fsend, frecv,
):
    lat = lax.axis_size("lat")
    me = lax.axis_index("lat")
    width = coef.shape[-1]
    spans = [(q * LANES, min(LANES, nlon - q * LANES)) for q in range(width // LANES)]
    rows = start_ref.shape[0]
    chunks = start_ref.shape[1] // 8
    has_lo = me > 0
    has_hi = me < lat - 1

    barrier = pltpu.get_barrier_semaphore()

    @pl.when(has_lo)
    def _():
        pl.semaphore_signal(barrier, inc=1, device_id={"lat": me - 1}, device_id_type=MESH)

    @pl.when(has_hi)
    def _():
        pl.semaphore_signal(barrier, inc=1, device_id={"lat": me + 1}, device_id_type=MESH)

    @pl.when(has_lo & has_hi)
    def _():
        pl.semaphore_wait(barrier, 2)

    @pl.when(jnp.logical_not(has_lo & has_hi))
    def _():
        pl.semaphore_wait(barrier, 1)

    def remote(src, dst, s, r, target):
        return pltpu.make_async_remote_copy(
            src_ref=src, dst_ref=dst, send_sem=s, recv_sem=r,
            device_id={"lat": target}, device_id_type=MESH,
        )

    def flows(up):
        far = me + 1 if up else me - 1
        base = 0 if up else 3
        n = rows - 1
        part = pl.ds(1, n) if up else pl.ds(0, n)
        dst_f, dst_l = (flow_lo, lev_lo) if up else (flow_hi, lev_hi)
        two = pl.ds(rows - 2, 2) if up else pl.ds(0, 2)
        return [
            remote(lev_ref, dst_l, fsend.at[base], frecv.at[base], far),
            remote(flow_ref.at[1, part], dst_f.at[1, part], fsend.at[base + 1], frecv.at[base + 1], far),
            remote(flow_ref.at[0, two], dst_f.at[0, two], fsend.at[base + 2], frecv.at[base + 2], far),
        ]

    def chunk(up, g):
        part = pl.ds(pl.multiple_of(g * 8, 8), 8)
        if up:
            return remote(start_ref.at[:, part], lo.at[:, part], send_up.at[g], recv_up.at[g], me + 1)
        return remote(start_ref.at[:, part], hi.at[:, part], send_dn.at[g], recv_dn.at[g], me - 1)

    @pl.when(has_hi)
    def _():
        for c in flows(True):
            c.start()

    @pl.when(has_lo)
    def _():
        for c in flows(False):
            c.start()

    def begin(g, carry):
        @pl.when(has_hi)
        def _():
            chunk(True, g).start()

        @pl.when(has_lo)
        def _():
            chunk(False, g).start()

        return carry

    lax.fori_loop(0, chunks, begin, 0)

    @pl.when(jnp.logical_not(has_lo))
    def _():
        flow_lo[...] = jnp.zeros_like(flow_lo)
        lev_lo[...] = jnp.zeros_like(lev_lo)
        lo[...] = jnp.zeros_like(lo)

    def tiles_of(x):
        x = jnp.concatenate([x, jnp.zeros((x.shape[0], width - nlon), x.dtype)], axis=1)
        return [x[:, q * LANES : (q + 1) * LANES] for q in range(width // LANES)]

    @pl.when(jnp.logical_not(has_hi))
    def _():
        for k in range(rows):
            src = rows - 1 - k
            piece = jnp.concatenate([flow_ref[0, src], flow_ref[1, src]], axis=0)
            for (at, n), t in zip(spans, mirrored(tiles_of(piece), nlon)):
                flow_hi[0, k, :, at : at + n] = -t[:levels, :n]
                flow_hi[1, k, :, at : at + n] = -t[levels:, :n]
            lev = jnp.broadcast_to(lev_ref[src : src + 1, :].astype(jnp.float32), (8, nlon))
            for (at, n), t in zip(spans, mirrored(tiles_of(lev), nlon)):
                lev_hi[k : k + 1, at : at + n] = (t[:1, :n] + 0.5).astype(jnp.int32)

        def fold(g, carry):
            part = pl.ds(pl.multiple_of(g * 8, 8), 8)
            x = jnp.concatenate([start_ref[rows - 1 - k, part, :] for k in range(rows)], axis=0)
            for (at, n), t in zip(spans, mirrored(tiles_of(x), nlon)):
                for k in range(rows):
                    hi[k, part, at : at + n] = t[8 * k : 8 * k + 8, :n]
            return carry

        lax.fori_loop(0, chunks, fold, 0)

    @pl.when(has_lo)
    def _():
        for c in flows(True):
            c.wait_recv()

    @pl.when(has_hi)
    def _():
        for c in flows(False):
            c.wait_recv()

    def pick(low, own, high, j):
        if j < 0:
            return low, j + rows
        if j < rows:
            return own, j
        return high, j - rows

    def shift(x, by):
        return pltpu.roll(x, (-by) % width, 1)

    ranks = lax.rem(lax.broadcasted_iota(jnp.int32, (8, nlon), 0), levels)

    for k in range(3 * rows):
        ref, at = pick(lev_lo, lev_ref, lev_hi, k - rows)
        lev = jnp.broadcast_to(ref[at : at + 1, :], (8, nlon))
        wets[k] = wrapped(jnp.where(ranks < lev, 1.0, 0.0), nlon)

    def wet_row(j):
        return wets[j + rows]

    def flow_row(which, j):
        ref, k = pick(flow_lo, flow_ref, flow_hi, j)
        return wrapped(jnp.concatenate([ref[which, k]] * (8 // levels), axis=0), nlon)

    def north_face(j):
        return face_terms(
            0.5 * (flow_row(1, j) + flow_row(1, j + 1)), wet_row(j) * wet_row(j + 1)
        )

    below = north_face(-3)
    for k in range(rows + 4):
        j = k - 2
        wet = wet_row(j)
        u = flow_row(0, j)
        ea, eb, ed, ee = face_terms(0.5 * (u + shift(u, 1)), wet * shift(wet, 1))
        above = north_face(j)
        coef[k, 0] = shift(ea, -1)
        coef[k, 1] = shift(eb, -1) - ea
        coef[k, 2] = shift(ee, -1) - ed
        coef[k, 3] = -ee
        coef[k, 4] = below[0]
        coef[k, 5] = below[1] - above[0]
        coef[k, 6] = below[3] - above[2]
        coef[k, 7] = -above[3]
        coef[k, 8] = 1.0 - eb + shift(ed, -1) - above[1] + below[2]
        below = above

    def section(get, k):
        f = get(0)
        total = coef[k, 8] * f
        total += coef[k, 0] * shift(f, -2)
        total += coef[k, 1] * shift(f, -1)
        total += coef[k, 2] * shift(f, 1)
        total += coef[k, 3] * shift(f, 2)
        total += coef[k, 4] * get(-2)
        total += coef[k, 5] * get(-1)
        total += coef[k, 6] * get(1)
        total += coef[k, 7] * get(2)
        return total

    def step(g, carry):
        @pl.when(has_lo)
        def _():
            chunk(True, g).wait_recv()

        @pl.when(has_hi)
        def _():
            chunk(False, g).wait_recv()

        part = pl.ds(pl.multiple_of(g * 8, 8), 8)

        for k in range(3 * rows):
            ref, at = pick(lo, start_ref, hi, k - rows)
            field[k] = wrapped(ref[at, part, :], nlon) * wets[k]
        for k in range(rows + 4):
            at = k + rows - 2
            first[k] = section(lambda d: field[at + d], k) * wets[at]
        for j in range(rows):
            second = section(lambda d: first[j + 2 + d], j + 2)
            value = 0.5 * (field[j + rows] + second) * wets[j + rows]
            out_ref[part, j, :] = value[:, :nlon]
        return carry

    lax.fori_loop(0, chunks, step, 0)

    @pl.when(has_hi)
    def _():
        for c in flows(True):
            c.wait_send()

    @pl.when(has_lo)
    def _():
        for c in flows(False):
            c.wait_send()

    def finish(g, carry):
        @pl.when(has_hi)
        def _():
            chunk(True, g).wait_send()

        @pl.when(has_lo)
        def _():
            chunk(False, g).wait_send()

        return carry

    lax.fori_loop(0, chunks, finish, 0)


def shards(tracers, currents, column_levels):
    count, levels, rows, nlon = tracers.shape
    width = -(-(nlon + 2 * WRAP) // LANES) * LANES
    start = jnp.transpose(tracers.reshape(count * levels, rows, nlon), (1, 0, 2))
    flow = jnp.transpose(currents, (0, 2, 1, 3))
    chunks = count * levels // 8
    vmem = pl.BlockSpec(memory_space=pltpu.VMEM)
    dma = pltpu.SemaphoreType.DMA
    out = pl.pallas_call(
        functools.partial(kernel, nlon, levels),
        out_shape=jax.ShapeDtypeStruct((count * levels, rows, nlon), jnp.float32),
        in_specs=[vmem] * 3,
        out_specs=vmem,
        scratch_shapes=[
            pltpu.VMEM(start.shape, jnp.float32),
            pltpu.VMEM(start.shape, jnp.float32),
            pltpu.VMEM(flow.shape, jnp.float32),
            pltpu.VMEM(flow.shape, jnp.float32),
            pltpu.VMEM(column_levels.shape, jnp.int32),
            pltpu.VMEM(column_levels.shape, jnp.int32),
            pltpu.VMEM((rows + 4, 9, 8, width), jnp.float32),
            pltpu.VMEM((3 * rows, 8, width), jnp.float32),
            pltpu.VMEM((3 * rows, 8, width), jnp.float32),
            pltpu.VMEM((rows + 4, 8, width), jnp.float32),
            dma((chunks,)), dma((chunks,)), dma((chunks,)), dma((chunks,)),
            dma((6,)), dma((6,)),
        ],
        compiler_params=pltpu.CompilerParams(
            collective_id=0, has_side_effects=True, vmem_limit_bytes=28 * 1024 * 1024
        ),
    )(start, flow, column_levels)
    return out.reshape(tracers.shape)


def solution(mesh):
    in_specs = (
        P("member", None, "lat", None),
        P("member", None, "lat", None),
        P(("member", "lat"), None),
    )
    out_specs = P("member", None, "lat", None)
    return jax.shard_map(shards, mesh=mesh, in_specs=in_specs, out_specs=out_specs, check_vma=False)
```

```python
import functools

import jax
import jax.numpy as jnp
from jax import lax
from jax.experimental import pallas as pl
from jax.experimental.pallas import tpu as pltpu
from jax.sharding import PartitionSpec as P

LANES = 128
WRAP = 4
MESH = pl.DeviceIdType.MESH


def wrapped(x, nlon):
    rest = nlon % LANES
    whole = nlon - rest
    tail = jnp.concatenate([x[:, whole:], x[:, : LANES - rest]], axis=1)
    lane = lax.broadcasted_iota(jnp.int32, tail.shape, 1)
    tail = jnp.where(lane >= LANES - WRAP, pltpu.roll(tail, LANES - rest, 1), tail)
    return jnp.concatenate([x[:, :whole], tail], axis=1)


def joined(main, pack, k, rest):
    lane = lax.broadcasted_iota(jnp.int32, pack.shape, 1)
    east = pltpu.roll(pack, (-k * rest) % LANES, 1)
    west = pltpu.roll(pack, (-(k + 1) * rest) % LANES, 1)
    tail = jnp.where(lane < rest, east, pltpu.roll(main[:, :LANES], rest, 1))
    tail = jnp.where(lane >= LANES - WRAP, west, tail)
    return jnp.concatenate([main, tail], axis=1)


def face_terms(c, opened):
    c = c * opened * (1.0 / 12.0)
    m = jnp.abs(c)
    return -c - m, 7.0 * c + 3.0 * m, 7.0 * c - 3.0 * m, m - c


def mirrored(tiles, nlon):
    count = len(tiles)
    rest = nlon % LANES
    row = lax.broadcasted_iota(jnp.int32, (LANES, LANES), 0)
    col = lax.broadcasted_iota(jnp.int32, (LANES, LANES), 1)
    near = jnp.where((row + col == rest - 1), 1.0, 0.0).astype(jnp.float32)
    far = jnp.where((row + col == LANES + rest - 1), 1.0, 0.0).astype(jnp.float32)
    dot = functools.partial(
        jnp.dot, precision=lax.Precision.HIGHEST, preferred_element_type=jnp.float32
    )
    return [
        dot(tiles[(count - 1 - q) % count], near) + dot(tiles[(count - 2 - q) % count], far)
        for q in range(count)
    ]


def kernel(
    nlon, levels, start_ref, flow_ref, lev_ref, out_ref,
    lo, hi, pack, pack_lo, pack_hi, flow_lo, flow_hi, lev_lo, lev_hi, coef, wets, field, first,
    send_up, recv_up, send_dn, recv_dn, fsend, frecv,
):
    lat = lax.axis_size("lat")
    me = lax.axis_index("lat")
    width = coef.shape[-1]
    spans = [(q * LANES, min(LANES, nlon - q * LANES)) for q in range(width // LANES)]
    rows = start_ref.shape[0]
    rest = nlon % LANES
    whole = nlon - rest
    chunks = start_ref.shape[1] // 8
    has_lo = me > 0
    has_hi = me < lat - 1

    barrier = pltpu.get_barrier_semaphore()

    @pl.when(has_lo)
    def _():
        pl.semaphore_signal(barrier, inc=1, device_id={"lat": me - 1}, device_id_type=MESH)

    @pl.when(has_hi)
    def _():
        pl.semaphore_signal(barrier, inc=1, device_id={"lat": me + 1}, device_id_type=MESH)

    for g in range(chunks):
        part = pl.ds(g * 8, 8)
        pack[part, :] = jnp.concatenate([start_ref[k, part, whole:] for k in range(rows)], axis=1)

    @pl.when(has_lo & has_hi)
    def _():
        pl.semaphore_wait(barrier, 2)

    @pl.when(jnp.logical_not(has_lo & has_hi))
    def _():
        pl.semaphore_wait(barrier, 1)

    def remote(src, dst, s, r, target):
        return pltpu.make_async_remote_copy(
            src_ref=src, dst_ref=dst, send_sem=s, recv_sem=r,
            device_id={"lat": target}, device_id_type=MESH,
        )

    def flows(up):
        far = me + 1 if up else me - 1
        base = 0 if up else 4
        dst_p = pack_lo if up else pack_hi
        n = rows - 1
        part = pl.ds(1, n) if up else pl.ds(0, n)
        dst_f, dst_l = (flow_lo, lev_lo) if up else (flow_hi, lev_hi)
        two = pl.ds(rows - 2, 2) if up else pl.ds(0, 2)
        return [
            remote(lev_ref, dst_l, fsend.at[base], frecv.at[base], far),
            remote(flow_ref.at[1, part], dst_f.at[1, part], fsend.at[base + 1], frecv.at[base + 1], far),
            remote(flow_ref.at[0, two], dst_f.at[0, two], fsend.at[base + 2], frecv.at[base + 2], far),
            remote(pack, dst_p, fsend.at[base + 3], frecv.at[base + 3], far),
        ]

    def chunk(up, g):
        part = pl.ds(pl.multiple_of(g * 8, 8), 8)
        main = start_ref.at[:, part, pl.ds(0, whole)]
        if up:
            return remote(main, lo.at[:, part], send_up.at[g], recv_up.at[g], me + 1)
        return remote(main, hi.at[:, part], send_dn.at[g], recv_dn.at[g], me - 1)

    @pl.when(has_hi)
    def _():
        for c in flows(True):
            c.start()

    @pl.when(has_lo)
    def _():
        for c in flows(False):
            c.start()

    def begin(g, carry):
        @pl.when(has_hi)
        def _():
            chunk(True, g).start()

        @pl.when(has_lo)
        def _():
            chunk(False, g).start()

        return carry

    lax.fori_loop(0, chunks, begin, 0)

    @pl.when(jnp.logical_not(has_lo))
    def _():
        flow_lo[...] = jnp.zeros_like(flow_lo)
        lev_lo[...] = jnp.zeros_like(lev_lo)
        lo[...] = jnp.zeros_like(lo)
        pack_lo[...] = jnp.zeros_like(pack_lo)

    def tiles_of(x):
        x = jnp.concatenate([x, jnp.zeros((x.shape[0], width - nlon), x.dtype)], axis=1)
        return [x[:, q * LANES : (q + 1) * LANES] for q in range(width // LANES)]

    @pl.when(jnp.logical_not(has_hi))
    def _():
        for k in range(rows):
            src = rows - 1 - k
            piece = jnp.concatenate([flow_ref[0, src], flow_ref[1, src]], axis=0)
            for (at, n), t in zip(spans, mirrored(tiles_of(piece), nlon)):
                flow_hi[0, k, :, at : at + n] = -t[:levels, :n]
                flow_hi[1, k, :, at : at + n] = -t[levels:, :n]
            lev = jnp.broadcast_to(lev_ref[src : src + 1, :].astype(jnp.float32), (8, nlon))
            for (at, n), t in zip(spans, mirrored(tiles_of(lev), nlon)):
                lev_hi[k : k + 1, at : at + n] = (t[:1, :n] + 0.5).astype(jnp.int32)

        def fold(g, carry):
            part = pl.ds(pl.multiple_of(g * 8, 8), 8)
            x = jnp.concatenate([start_ref[rows - 1 - k, part, :] for k in range(rows)], axis=0)
            tiles = mirrored(tiles_of(x), nlon)
            for (at, n), t in zip(spans[:-1], tiles[:-1]):
                for k in range(rows):
                    hi[k, part, at : at + n] = t[8 * k : 8 * k + 8, :n]
            ends = [tiles[-1][8 * k : 8 * k + 8, :rest] for k in range(rows)]
            pack_hi[part, :] = jnp.concatenate(ends, axis=1)
            return carry

        lax.fori_loop(0, chunks, fold, 0)

    @pl.when(has_lo)
    def _():
        for c in flows(True):
            c.wait_recv()

    @pl.when(has_hi)
    def _():
        for c in flows(False):
            c.wait_recv()

    def pick(low, own, high, j):
        if j < 0:
            return low, j + rows
        if j < rows:
            return own, j
        return high, j - rows

    def shift(x, by):
        return pltpu.roll(x, (-by) % width, 1)

    ranks = lax.rem(lax.broadcasted_iota(jnp.int32, (8, nlon), 0), levels)

    for k in range(3 * rows):
        ref, at = pick(lev_lo, lev_ref, lev_hi, k - rows)
        lev = jnp.broadcast_to(ref[at : at + 1, :], (8, nlon))
        wets[k] = wrapped(jnp.where(ranks < lev, 1.0, 0.0), nlon)

    def wet_row(j):
        return wets[j + rows]

    def flow_row(which, j):
        ref, k = pick(flow_lo, flow_ref, flow_hi, j)
        return wrapped(jnp.concatenate([ref[which, k]] * (8 // levels), axis=0), nlon)

    def north_face(j):
        return face_terms(
            0.5 * (flow_row(1, j) + flow_row(1, j + 1)), wet_row(j) * wet_row(j + 1)
        )

    below = north_face(-3)
    for k in range(rows + 4):
        j = k - 2
        wet = wet_row(j)
        u = flow_row(0, j)
        ea, eb, ed, ee = face_terms(0.5 * (u + shift(u, 1)), wet * shift(wet, 1))
        above = north_face(j)
        coef[k, 0] = shift(ea, -1)
        coef[k, 1] = shift(eb, -1) - ea
        coef[k, 2] = shift(ee, -1) - ed
        coef[k, 3] = -ee
        coef[k, 4] = below[0]
        coef[k, 5] = below[1] - above[0]
        coef[k, 6] = below[3] - above[2]
        coef[k, 7] = -above[3]
        coef[k, 8] = 1.0 - eb + shift(ed, -1) - above[1] + below[2]
        below = above

    def section(get, k):
        f = get(0)
        total = coef[k, 8] * f
        total += coef[k, 0] * shift(f, -2)
        total += coef[k, 1] * shift(f, -1)
        total += coef[k, 2] * shift(f, 1)
        total += coef[k, 3] * shift(f, 2)
        total += coef[k, 4] * get(-2)
        total += coef[k, 5] * get(-1)
        total += coef[k, 6] * get(1)
        total += coef[k, 7] * get(2)
        return total

    def step(g, carry):
        @pl.when(has_lo)
        def _():
            chunk(True, g).wait_recv()

        @pl.when(has_hi)
        def _():
            chunk(False, g).wait_recv()

        part = pl.ds(pl.multiple_of(g * 8, 8), 8)

        for k in range(3 * rows):
            ref, at = pick(lo, start_ref, hi, k - rows)
            ends, _ = pick(pack_lo, pack, pack_hi, k - rows)
            field[k] = joined(ref[at, part, :whole], ends[part, :], at, rest) * wets[k]
        for k in range(rows + 4):
            at = k + rows - 2
            first[k] = section(lambda d: field[at + d], k) * wets[at]
        for j in range(rows):
            second = section(lambda d: first[j + 2 + d], j + 2)
            value = 0.5 * (field[j + rows] + second) * wets[j + rows]
            out_ref[part, j, :] = value[:, :nlon]
        return carry

    lax.fori_loop(0, chunks, step, 0)

    @pl.when(has_hi)
    def _():
        for c in flows(True):
            c.wait_send()

    @pl.when(has_lo)
    def _():
        for c in flows(False):
            c.wait_send()

    def finish(g, carry):
        @pl.when(has_hi)
        def _():
            chunk(True, g).wait_send()

        @pl.when(has_lo)
        def _():
            chunk(False, g).wait_send()

        return carry

    lax.fori_loop(0, chunks, finish, 0)


def shards(tracers, currents, column_levels):
    count, levels, rows, nlon = tracers.shape
    width = -(-(nlon + 2 * WRAP) // LANES) * LANES
    start = jnp.transpose(tracers.reshape(count * levels, rows, nlon), (1, 0, 2))
    flow = jnp.transpose(currents, (0, 2, 1, 3))
    chunks = count * levels // 8
    vmem = pl.BlockSpec(memory_space=pltpu.VMEM)
    dma = pltpu.SemaphoreType.DMA
    out = pl.pallas_call(
        functools.partial(kernel, nlon, levels),
        out_shape=jax.ShapeDtypeStruct((count * levels, rows, nlon), jnp.float32),
        in_specs=[vmem] * 3,
        out_specs=vmem,
        scratch_shapes=[
            pltpu.VMEM((rows, count * levels, nlon - nlon % LANES), jnp.float32),
            pltpu.VMEM((rows, count * levels, nlon - nlon % LANES), jnp.float32),
            pltpu.VMEM((count * levels, LANES), jnp.float32),
            pltpu.VMEM((count * levels, LANES), jnp.float32),
            pltpu.VMEM((count * levels, LANES), jnp.float32),
            pltpu.VMEM(flow.shape, jnp.float32),
            pltpu.VMEM(flow.shape, jnp.float32),
            pltpu.VMEM(column_levels.shape, jnp.int32),
            pltpu.VMEM(column_levels.shape, jnp.int32),
            pltpu.VMEM((rows + 4, 9, 8, width), jnp.float32),
            pltpu.VMEM((3 * rows, 8, width), jnp.float32),
            pltpu.VMEM((3 * rows, 8, width), jnp.float32),
            pltpu.VMEM((rows + 4, 8, width), jnp.float32),
            dma((chunks,)), dma((chunks,)), dma((chunks,)), dma((chunks,)),
            dma((8,)), dma((8,)),
        ],
        compiler_params=pltpu.CompilerParams(
            collective_id=0, has_side_effects=True, vmem_limit_bytes=28 * 1024 * 1024
        ),
    )(start, flow, column_levels)
    return out.reshape(tracers.shape)


def solution(mesh):
    in_specs = (
        P("member", None, "lat", None),
        P("member", None, "lat", None),
        P(("member", "lat"), None),
    )
    out_specs = P("member", None, "lat", None)
    return jax.shard_map(shards, mesh=mesh, in_specs=in_specs, out_specs=out_specs, check_vma=False)
```

```python
import functools

import jax
import jax.numpy as jnp
from jax import lax
from jax.experimental import pallas as pl
from jax.experimental.pallas import tpu as pltpu
from jax.sharding import PartitionSpec as P

LANES = 128
WRAP = 4
MESH = pl.DeviceIdType.MESH


def wrapped(x, nlon):
    rest = nlon % LANES
    whole = nlon - rest
    tail = jnp.concatenate([x[:, whole:], x[:, : LANES - rest]], axis=1)
    lane = lax.broadcasted_iota(jnp.int32, tail.shape, 1)
    tail = jnp.where(lane >= LANES - WRAP, pltpu.roll(tail, LANES - rest, 1), tail)
    return jnp.concatenate([x[:, :whole], tail], axis=1)


def joined(main, pack, k, rest):
    lane = lax.broadcasted_iota(jnp.int32, pack.shape, 1)
    east = pltpu.roll(pack, (-k * rest) % LANES, 1)
    west = pltpu.roll(pack, (-(k + 1) * rest) % LANES, 1)
    tail = jnp.where(lane < rest, east, pltpu.roll(main[:, :LANES], rest, 1))
    tail = jnp.where(lane >= LANES - WRAP, west, tail)
    return jnp.concatenate([main, tail], axis=1)


def face_terms(c, opened):
    c = c * opened * (1.0 / 12.0)
    m = jnp.abs(c)
    return -c - m, 7.0 * c + 3.0 * m, 7.0 * c - 3.0 * m, m - c


def mirrored(tiles, nlon):
    count = len(tiles)
    rest = nlon % LANES
    row = lax.broadcasted_iota(jnp.int32, (LANES, LANES), 0)
    col = lax.broadcasted_iota(jnp.int32, (LANES, LANES), 1)
    near = jnp.where((row + col == rest - 1), 1.0, 0.0).astype(jnp.float32)
    far = jnp.where((row + col == LANES + rest - 1), 1.0, 0.0).astype(jnp.float32)
    dot = functools.partial(
        jnp.dot, precision=lax.Precision.HIGHEST, preferred_element_type=jnp.float32
    )
    return [
        dot(tiles[(count - 1 - q) % count], near) + dot(tiles[(count - 2 - q) % count], far)
        for q in range(count)
    ]


def kernel(
    nlon, levels, raw_ref, raw_flow, lev_ref, out_ref,
    start_ref, flow_ref, lo, hi, pack, pack_lo, pack_hi, flow_lo, flow_hi, lev_lo, lev_hi, coef, wets, field, first,
    send_up, recv_up, send_dn, recv_dn, fsend, frecv,
):
    lat = lax.axis_size("lat")
    me = lax.axis_index("lat")
    width = coef.shape[-1]
    spans = [(q * LANES, min(LANES, nlon - q * LANES)) for q in range(width // LANES)]
    rows = start_ref.shape[0]
    rest = nlon % LANES
    whole = nlon - rest
    chunks = start_ref.shape[1] // 8
    has_lo = me > 0
    has_hi = me < lat - 1

    barrier = pltpu.get_barrier_semaphore()

    @pl.when(has_lo)
    def _():
        pl.semaphore_signal(barrier, inc=1, device_id={"lat": me - 1}, device_id_type=MESH)

    @pl.when(has_hi)
    def _():
        pl.semaphore_signal(barrier, inc=1, device_id={"lat": me + 1}, device_id_type=MESH)

    for g in range(chunks):
        part = pl.ds(g * 8, 8)
        pack[part, :] = jnp.concatenate([raw_ref[part, k, whole:] for k in range(rows)], axis=1)

    for k in range(rows):
        for which in range(2):
            flow_ref[which, k] = raw_flow[which, :, k, :]

    def reorder(g):
        part = pl.ds(pl.multiple_of(g * 8, 8), 8)
        for k in range(rows):
            start_ref[k, part, :] = raw_ref[part, k, :]

    reorder(0)

    @pl.when(has_lo & has_hi)
    def _():
        pl.semaphore_wait(barrier, 2)

    @pl.when(jnp.logical_not(has_lo & has_hi))
    def _():
        pl.semaphore_wait(barrier, 1)

    def remote(src, dst, s, r, target):
        return pltpu.make_async_remote_copy(
            src_ref=src, dst_ref=dst, send_sem=s, recv_sem=r,
            device_id={"lat": target}, device_id_type=MESH,
        )

    def flows(up):
        far = me + 1 if up else me - 1
        base = 0 if up else 4
        dst_p = pack_lo if up else pack_hi
        n = rows - 1
        part = pl.ds(1, n) if up else pl.ds(0, n)
        dst_f, dst_l = (flow_lo, lev_lo) if up else (flow_hi, lev_hi)
        two = pl.ds(rows - 2, 2) if up else pl.ds(0, 2)
        return [
            remote(lev_ref, dst_l, fsend.at[base], frecv.at[base], far),
            remote(flow_ref.at[1, part], dst_f.at[1, part], fsend.at[base + 1], frecv.at[base + 1], far),
            remote(flow_ref.at[0, two], dst_f.at[0, two], fsend.at[base + 2], frecv.at[base + 2], far),
            remote(pack, dst_p, fsend.at[base + 3], frecv.at[base + 3], far),
        ]

    def chunk(up, g):
        part = pl.ds(pl.multiple_of(g * 8, 8), 8)
        main = start_ref.at[:, part, pl.ds(0, whole)]
        if up:
            return remote(main, lo.at[:, part], send_up.at[g], recv_up.at[g], me + 1)
        return remote(main, hi.at[:, part], send_dn.at[g], recv_dn.at[g], me - 1)

    @pl.when(has_hi)
    def _():
        for c in flows(True):
            c.start()

    @pl.when(has_lo)
    def _():
        for c in flows(False):
            c.start()

    def begin(g, carry):
        @pl.when(g < chunks - 1)
        def _():
            reorder(g + 1)

        @pl.when(has_hi)
        def _():
            chunk(True, g).start()

        @pl.when(has_lo)
        def _():
            chunk(False, g).start()

        return carry

    lax.fori_loop(0, chunks, begin, 0)

    @pl.when(jnp.logical_not(has_lo))
    def _():
        flow_lo[...] = jnp.zeros_like(flow_lo)
        lev_lo[...] = jnp.zeros_like(lev_lo)
        lo[...] = jnp.zeros_like(lo)
        pack_lo[...] = jnp.zeros_like(pack_lo)

    def tiles_of(x):
        x = jnp.concatenate([x, jnp.zeros((x.shape[0], width - nlon), x.dtype)], axis=1)
        return [x[:, q * LANES : (q + 1) * LANES] for q in range(width // LANES)]

    @pl.when(jnp.logical_not(has_hi))
    def _():
        for k in range(rows):
            src = rows - 1 - k
            piece = jnp.concatenate([flow_ref[0, src], flow_ref[1, src]], axis=0)
            for (at, n), t in zip(spans, mirrored(tiles_of(piece), nlon)):
                flow_hi[0, k, :, at : at + n] = -t[:levels, :n]
                flow_hi[1, k, :, at : at + n] = -t[levels:, :n]
            lev = jnp.broadcast_to(lev_ref[src : src + 1, :].astype(jnp.float32), (8, nlon))
            for (at, n), t in zip(spans, mirrored(tiles_of(lev), nlon)):
                lev_hi[k : k + 1, at : at + n] = (t[:1, :n] + 0.5).astype(jnp.int32)

        def fold(g, carry):
            part = pl.ds(pl.multiple_of(g * 8, 8), 8)
            x = jnp.concatenate([start_ref[rows - 1 - k, part, :] for k in range(rows)], axis=0)
            tiles = mirrored(tiles_of(x), nlon)
            for (at, n), t in zip(spans[:-1], tiles[:-1]):
                for k in range(rows):
                    hi[k, part, at : at + n] = t[8 * k : 8 * k + 8, :n]
            ends = [tiles[-1][8 * k : 8 * k + 8, :rest] for k in range(rows)]
            pack_hi[part, :] = jnp.concatenate(ends, axis=1)
            return carry

        lax.fori_loop(0, chunks, fold, 0)

    @pl.when(has_lo)
    def _():
        for c in flows(True):
            c.wait_recv()

    @pl.when(has_hi)
    def _():
        for c in flows(False):
            c.wait_recv()

    def pick(low, own, high, j):
        if j < 0:
            return low, j + rows
        if j < rows:
            return own, j
        return high, j - rows

    def shift(x, by):
        return pltpu.roll(x, (-by) % width, 1)

    ranks = lax.rem(lax.broadcasted_iota(jnp.int32, (8, nlon), 0), levels)

    for k in range(3 * rows):
        ref, at = pick(lev_lo, lev_ref, lev_hi, k - rows)
        lev = jnp.broadcast_to(ref[at : at + 1, :], (8, nlon))
        wets[k] = wrapped(jnp.where(ranks < lev, 1.0, 0.0), nlon)

    def wet_row(j):
        return wets[j + rows]

    def flow_row(which, j):
        ref, k = pick(flow_lo, flow_ref, flow_hi, j)
        return wrapped(jnp.concatenate([ref[which, k]] * (8 // levels), axis=0), nlon)

    def north_face(j):
        return face_terms(
            0.5 * (flow_row(1, j) + flow_row(1, j + 1)), wet_row(j) * wet_row(j + 1)
        )

    below = north_face(-3)
    for k in range(rows + 4):
        j = k - 2
        wet = wet_row(j)
        u = flow_row(0, j)
        ea, eb, ed, ee = face_terms(0.5 * (u + shift(u, 1)), wet * shift(wet, 1))
        above = north_face(j)
        coef[k, 0] = shift(ea, -1)
        coef[k, 1] = shift(eb, -1) - ea
        coef[k, 2] = shift(ee, -1) - ed
        coef[k, 3] = -ee
        coef[k, 4] = below[0]
        coef[k, 5] = below[1] - above[0]
        coef[k, 6] = below[3] - above[2]
        coef[k, 7] = -above[3]
        coef[k, 8] = 1.0 - eb + shift(ed, -1) - above[1] + below[2]
        below = above

    def section(get, k):
        f = get(0)
        total = coef[k, 8] * f
        total += coef[k, 0] * shift(f, -2)
        total += coef[k, 1] * shift(f, -1)
        total += coef[k, 2] * shift(f, 1)
        total += coef[k, 3] * shift(f, 2)
        total += coef[k, 4] * get(-2)
        total += coef[k, 5] * get(-1)
        total += coef[k, 6] * get(1)
        total += coef[k, 7] * get(2)
        return total

    def step(g, carry):
        @pl.when(has_lo)
        def _():
            chunk(True, g).wait_recv()

        @pl.when(has_hi)
        def _():
            chunk(False, g).wait_recv()

        part = pl.ds(pl.multiple_of(g * 8, 8), 8)

        for k in range(3 * rows):
            ref, at = pick(lo, start_ref, hi, k - rows)
            ends, _ = pick(pack_lo, pack, pack_hi, k - rows)
            field[k] = joined(ref[at, part, :whole], ends[part, :], at, rest) * wets[k]
        for k in range(rows + 4):
            at = k + rows - 2
            first[k] = section(lambda d: field[at + d], k) * wets[at]
        for j in range(rows):
            second = section(lambda d: first[j + 2 + d], j + 2)
            value = 0.5 * (field[j + rows] + second) * wets[j + rows]
            out_ref[part, j, :] = value[:, :nlon]
        return carry

    lax.fori_loop(0, chunks, step, 0)

    @pl.when(has_hi)
    def _():
        for c in flows(True):
            c.wait_send()

    @pl.when(has_lo)
    def _():
        for c in flows(False):
            c.wait_send()

    def finish(g, carry):
        @pl.when(has_hi)
        def _():
            chunk(True, g).wait_send()

        @pl.when(has_lo)
        def _():
            chunk(False, g).wait_send()

        return carry

    lax.fori_loop(0, chunks, finish, 0)


def shards(tracers, currents, column_levels):
    count, levels, rows, nlon = tracers.shape
    width = -(-(nlon + 2 * WRAP) // LANES) * LANES
    raw = tracers.reshape(count * levels, rows, nlon)
    chunks = count * levels // 8
    vmem = pl.BlockSpec(memory_space=pltpu.VMEM)
    dma = pltpu.SemaphoreType.DMA
    out = pl.pallas_call(
        functools.partial(kernel, nlon, levels),
        out_shape=jax.ShapeDtypeStruct((count * levels, rows, nlon), jnp.float32),
        in_specs=[vmem] * 3,
        out_specs=vmem,
        scratch_shapes=[
            pltpu.VMEM((rows, count * levels, nlon), jnp.float32),
            pltpu.VMEM((2, rows, levels, nlon), jnp.float32),
            pltpu.VMEM((rows, count * levels, nlon - nlon % LANES), jnp.float32),
            pltpu.VMEM((rows, count * levels, nlon - nlon % LANES), jnp.float32),
            pltpu.VMEM((count * levels, LANES), jnp.float32),
            pltpu.VMEM((count * levels, LANES), jnp.float32),
            pltpu.VMEM((count * levels, LANES), jnp.float32),
            pltpu.VMEM((2, rows, levels, nlon), jnp.float32),
            pltpu.VMEM((2, rows, levels, nlon), jnp.float32),
            pltpu.VMEM(column_levels.shape, jnp.int32),
            pltpu.VMEM(column_levels.shape, jnp.int32),
            pltpu.VMEM((rows + 4, 9, 8, width), jnp.float32),
            pltpu.VMEM((3 * rows, 8, width), jnp.float32),
            pltpu.VMEM((3 * rows, 8, width), jnp.float32),
            pltpu.VMEM((rows + 4, 8, width), jnp.float32),
            dma((chunks,)), dma((chunks,)), dma((chunks,)), dma((chunks,)),
            dma((8,)), dma((8,)),
        ],
        compiler_params=pltpu.CompilerParams(
            collective_id=0, has_side_effects=True, vmem_limit_bytes=28 * 1024 * 1024
        ),
    )(raw, currents, column_levels)
    return out.reshape(tracers.shape)


def solution(mesh):
    in_specs = (
        P("member", None, "lat", None),
        P("member", None, "lat", None),
        P(("member", "lat"), None),
    )
    out_specs = P("member", None, "lat", None)
    return jax.shard_map(shards, mesh=mesh, in_specs=in_specs, out_specs=out_specs, check_vma=False)
```
